32 devices in a mesh: dp: 1 (over z), ing: 4 (over y), grp: 8 (over x, core).
Axes of the slice: x: 4, y: 4, z: 1, core: 2. Of those that a mesh axis runs over, the one named last changes fastest.
The devices are a block of a 4x4x8 slice.
Arguments:
- x: bfloat16 [16384, 2048], P(('dp', 'grp', 'ing'))
- idx: int32 [16384, 3, 2], P(('dp', 'grp', 'ing'))
- g: float32 [16384, 3, 2], P(('dp', 'grp', 'ing'))
- w1: bfloat16 [64, 2048, 1408], P(('grp', 'ing'))
- w3: bfloat16 [64, 2048, 1408], P(('grp', 'ing'))
- w2: bfloat16 [64, 1408, 2048], P(('grp', 'ing'))
- s1: bfloat16 [2048, 2816], replicated
- s3: bfloat16 [2048, 2816], replicated
- s2: bfloat16 [2816, 2048], replicated
Outputs:
- output: bfloat16 [16384, 2048], P(('dp', 'grp', 'ing'))
All inputs are finite; a program needn't handle non-finite values.
Results may differ from the reference program's by a relative error of at most 0.00112.
Values are sent between devices in bfloat16 or wider.
A program may use at most 768 MiB of HBM per device.

```python
import jax
import jax.numpy as jnp
from jax import lax

T = 512
D = 2048
F = 1408
FS = 2816
E = 64
K = 6
M = 3
GRP = 8
ING = 4

N = GRP * ING
EG = E // GRP
KG = K // M
C = (3 * T * K + 2 * E - 1) // (2 * E)


def _route(key, sizes, tau):
    kr, ks = jax.random.split(key)
    s = jnp.array(sizes, dtype=jnp.int32)
    ends = jnp.cumsum(s)
    r = jax.random.permutation(kr, T)
    o = jnp.searchsorted(ends, r, side='right')
    w = r - (ends - s)[o]
    sig = jax.vmap(lambda kk: jax.random.permutation(kk, EG))(jax.random.split(ks, GRP))
    cols = []
    for m in range(M):
        pos = w
        for mp in range(m):
            pos = pos + s[(o + m - mp) % GRP]
        lab = tau[(o + m) % GRP][:, None]
        loc = (pos[:, None] * KG + jnp.arange(KG)[None, :]) % EG
        cols.append(lab * EG + sig[lab, loc])
    return jnp.stack(cols, axis=1).astype(jnp.int32)


def _experts(key, shape, scale):
    return lax.map(lambda k: (jax.random.normal(k, shape, jnp.float32) * scale).astype(jnp.bfloat16), jax.random.split(key, E))


def setup_inputs(seed: int = 0, part: int = 0) -> dict:
    key = jax.random.PRNGKey(seed)
    kw, kp = jax.random.split(key)
    k1, k2, k3, k4, k5, k6 = jax.random.split(kw, 6)
    kpp = jax.random.fold_in(kp, part)
    kx, _, _, kg = jax.random.split(kpp, 4)
    kr, kt = jax.random.split(jax.random.fold_in(kpp, 7))
    sizes = [3 * T // (2 * GRP)] * (GRP // 2) + [T // (2 * GRP)] * (GRP // 2)
    tau = jax.random.permutation(kt, GRP)
    idx = jax.vmap(lambda kk: _route(kk, sizes, tau))(jax.random.split(kr, N))
    g = jax.nn.softmax(0.8 * jax.random.normal(kg, (N * T, K), jnp.float32), axis=-1)
    return {
        'x': jax.random.normal(kx, (N * T, D), jnp.float32).astype(jnp.bfloat16),
        'idx': idx.reshape(N * T, M, KG),
        'g': g.reshape(N * T, M, KG),
        'w1': _experts(k1, (D, F), D ** -0.5),
        'w3': _experts(k2, (D, F), D ** -0.5),
        'w2': _experts(k3, (F, D), F ** -0.5),
        's1': (jax.random.normal(k4, (D, FS), jnp.float32) * D ** -0.5).astype(jnp.bfloat16),
        's3': (jax.random.normal(k5, (D, FS), jnp.float32) * D ** -0.5).astype(jnp.bfloat16),
        's2': (jax.random.normal(k6, (FS, D), jnp.float32) * FS ** -0.5).astype(jnp.bfloat16),
    }


def _swiglu(v, a, b, c):
    h1 = jnp.dot(v, a, preferred_element_type=jnp.float32)
    h3 = jnp.dot(v, b, preferred_element_type=jnp.float32)
    h = (jax.nn.silu(h1) * h3).astype(jnp.bfloat16)
    return jnp.dot(h, c, preferred_element_type=jnp.float32)


def reference(x, idx, g, w1, w3, w2, s1, s3, s2):
    nt = x.shape[0]
    flat = idx.reshape(nt, K)
    gf = g.reshape(nt, K)

    def expert(acc, xs):
        e, a, b, c = xs
        hit = flat == e
        wt = jnp.sum(jnp.where(hit, gf, 0.0), axis=1)
        rows = jnp.nonzero(jnp.any(hit, axis=1), size=N * C, fill_value=nt)[0]
        xe = jnp.take(x, rows, axis=0, mode='fill', fill_value=0)
        out = _swiglu(xe, a, b, c).astype(jnp.bfloat16).astype(jnp.float32)
        we = jnp.take(wt, rows, mode='fill', fill_value=0)
        return acc.at[rows].add(we[:, None] * out, mode='drop'), None

    def group(tot, xs):
        b, a1, a3, a2 = xs
        acc, _ = lax.scan(expert, jnp.zeros((nt, D), jnp.float32), (b * EG + jnp.arange(EG), a1, a3, a2))
        return tot + acc.astype(jnp.bfloat16).astype(jnp.float32), None

    tot, _ = lax.scan(group, jnp.zeros((nt, D), jnp.float32),
                      (jnp.arange(GRP), w1.reshape(GRP, EG, D, F), w3.reshape(GRP, EG, D, F), w2.reshape(GRP, EG, F, D)))
    return (tot + _swiglu(x, s1, s3, s2)).astype(jnp.bfloat16)
```

```python
import functools

import jax
import jax.numpy as jnp
from jax import lax
from jax.experimental import pallas as pl
from jax.experimental.pallas import tpu as pltpu
from jax.sharding import PartitionSpec as P

MESH = pl.DeviceIdType.MESH
LANES = 128


def _moe_kernel(G, n, EL, C, CG, T, D, F, K,
                x_ref, it_ref, gt_ref, ic_ref, w1_ref, w3_ref, w2_ref, s1_ref, s3_ref, s2_ref,
                y_ref, pr, xg, xs, xr, es, er, ps,
                W1, W3, W2, xb, eb, rb, pb, fb, hb, xgv, selv, putv, wqv, acc, tri, cvec,
                icv, idxy, idxx, gx,
                agS, agR, iyS, iyR, ixS, ixR, gxS, gxR, xS, xR, eS, eR, pS, pR, lsem, wsem):
    EG = EL * n
    CB = EL * C
    R = n * CB
    RE = n * C
    M = K // 2
    H = T // 2
    NB = min(256, D)
    LAG = 4
    bf = jnp.bfloat16
    f32 = jnp.float32
    i32 = jnp.int32
    d = lax.axis_index('dp')
    j = lax.axis_index('ing')
    b = lax.axis_index('grp')
    chips = G // 2
    chip, core = b // 2, b % 2

    def grp_at(s):
        q, r = s // 2, s % 2
        mid = ((q + 1) // 2) % 2
        dc = mid * (1 + 2 * r) + (q // 3) * 2
        dcore = (1 - mid) * r + mid * (q - 1)
        return 2 * ((chip + dc) % chips) + (core + dcore) % 2

    def inv(s):
        q, r = s // 2, s % 2
        mid = ((q + 1) // 2) % 2
        return 2 * q + r + mid * (1 - 2 * r)

    def xdev(s):
        return (d, j, grp_at(s))

    def ydev(k):
        return (d, (j + k) % n, b)

    def iota(shape, dim):
        return lax.broadcasted_iota(i32, shape, dim)

    def remote(src, dst, ss, rs, dev):
        return pltpu.make_async_remote_copy(src_ref=src, dst_ref=dst, send_sem=ss, recv_sem=rs,
                                            device_id=dev, device_id_type=MESH)

    barrier = pltpu.get_barrier_semaphore()
    for k in range(1, n):
        pl.semaphore_signal(barrier, 1, device_id=ydev(k), device_id_type=MESH)
    for s in range(1, G):
        pl.semaphore_signal(barrier, 1, device_id=xdev(s), device_id_type=MESH)
    pl.semaphore_wait(barrier, n - 1 + G - 1)

    def ag(k):
        return remote(x_ref, xg.at[k], agS.at[k], agR.at[k], ydev(n - k))

    def fwd(h):
        k, dev = (1, n - 1) if h == 0 else (n - 1, 1)
        rows = pl.ds(h * H, H)
        return remote(xg.at[k, rows], xg.at[2, rows], agS.at[2 * h], agR.at[2 * h], ydev(dev))

    def iy(k):
        return remote(it_ref, idxy.at[k], iyS.at[k], iyR.at[k], ydev(n - k))

    def ix(s):
        return remote(it_ref, idxx.at[inv(s)], ixS.at[s], ixR.at[inv(s)], xdev(s))

    def ixrecv(s):
        return remote(it_ref, idxx.at[s], ixS.at[s], ixR.at[s], xdev(s))

    def gxc(s):
        return remote(gt_ref, gx.at[inv(s)], gxS.at[s], gxR.at[inv(s)], xdev(s))

    def gxrecv(s):
        return remote(gt_ref, gx.at[s], gxS.at[s], gxR.at[s], xdev(s))

    def xcopy(s, k):
        return remote(xs.at[k, grp_at(s)], xr.at[inv(s), k], xS.at[s, k], xR.at[inv(s), k], xdev(s))

    def xrecv(s, k):
        return remote(xs.at[k, grp_at(s)], xr.at[s, k], xS.at[s, k], xR.at[s, k], xdev(s))

    def ecopy(s, k):
        return remote(es.at[s, k], er.at[s, n - k], eS.at[s, k], eR.at[s, n - k], ydev(k))

    def erecv(s, k):
        return remote(es.at[s, k], er.at[s, k], eS.at[s, k], eR.at[s, k], ydev(k))

    def pcopy(s):
        return remote(ps.at[s], pr.at[b], pS.at[s], pR.at[b], xdev(s))

    def precv(s):
        g = grp_at(s)
        return remote(ps.at[s], pr.at[g], pS.at[s], pR.at[g], xdev(s))

    def run(copies):
        for c in copies:
            c.start()
        for c in copies:
            c.wait()

    for k in range(1, n):
        iy(k).start()
    ag(1).start()
    ag(n - 1).start()

    def weights(l, shared):
        cols = pl.ds(l * F, F)
        srcs = ((s1_ref.at[:, cols], s3_ref.at[:, cols], s2_ref.at[cols]) if shared
                else (w1_ref.at[l], w3_ref.at[l], w2_ref.at[l]))
        return [pltpu.make_async_copy(s, w.at[l], wsem.at[l, i])
                for i, (s, w) in enumerate(zip(srcs, (W1, W3, W2)))]

    run([pltpu.make_async_copy(it_ref, idxy.at[0], lsem.at[0]),
         pltpu.make_async_copy(it_ref, idxx.at[0], lsem.at[1]),
         pltpu.make_async_copy(gt_ref, gx.at[0], lsem.at[2]),
         pltpu.make_async_copy(ic_ref, icv, lsem.at[3]),
         pltpu.make_async_copy(x_ref, xgv, lsem.at[4])])
    for s in range(1, G):
        ix(s).start()
        gxc(s).start()
    for l in range(EL):
        for c in weights(l, True):
            c.start()
    tri[...] = (iota((T, T), 0) < iota((T, T), 1)).astype(f32).astype(bf)

    def one_hot_rows(iv, eid):
        oh = iv[0:1, :] == eid
        for i in range(1, K):
            oh = oh | (iv[i:i + 1, :] == eid)
        return oh

    def gather(k):
        iv = idxy[k]
        r = iota((G * EL, T), 0)
        g_of = jnp.zeros((G * EL, T), i32)
        for q in range(1, G):
            g_of = g_of + (r >= q * EL).astype(i32)
        eid = g_of * (EG - EL) + r + j * EL
        oh = one_hot_rows(iv, eid)
        rank = jnp.dot(oh.astype(f32).astype(bf), tri[...], preferred_element_type=f32)
        code = jnp.where(oh, rank.astype(i32), -(EL * C))
        row = iota((CB, T), 0)
        for g in range(G):
            want = code[g * EL:g * EL + 1, :]
            for l in range(1, EL):
                want = jnp.where(row < l * C, want, code[g * EL + l:g * EL + l + 1, :] + l * C)
            selv[g * CB:(g + 1) * CB, :] = (row == want).astype(f32).astype(bf)

        def col(i, _):
            cols = pl.ds(pl.multiple_of(i * NB, NB), NB)
            xb[:, cols] = jnp.dot(selv[...], xgv[:, cols], preferred_element_type=f32).astype(bf)
            return 0

        lax.fori_loop(0, D // NB, col, 0)
        run([pltpu.make_async_copy(xb.at[pl.ds(g * CB, CB)], xs.at[k, g], lsem.at[g]) for g in range(G)]
            + [pltpu.make_async_copy(xb.at[pl.ds(pl.multiple_of(b * CB, 8), CB)], xr.at[0, k], lsem.at[G])])

    def fetch(k):
        run([pltpu.make_async_copy(xg.at[k], xgv, lsem.at[0])])

    def up(l, src, rows, m):
        def body(i, _):
            cols = pl.ds(pl.multiple_of(i * LANES, LANES), LANES)
            w = jnp.concatenate([W1[l, :, cols], W3[l, :, cols]], axis=1)
            hh = jnp.dot(src[rows, :], w, preferred_element_type=f32)
            a, c = hh[:, :LANES], hh[:, LANES:]
            hb[0:m, cols] = (a * jax.nn.sigmoid(a) * c).astype(bf)
            return 0

        lax.fori_loop(0, F // LANES, body, 0)

    gather(0)
    for s in range(1, G):
        xcopy(s, 0).start()

    lane = iota((T, LANES), 1)
    hit = jnp.zeros((T, LANES), i32)
    for m in range(M):
        v = icv[:, 2 * m:2 * m + 1]
        hit = hit + ((v >= lane * EG) & (v < lane * EG + EG)).astype(i32)
    below = lax.dot_general(tri[...], hit.astype(f32).astype(bf), (((0,), (0,)), ((), ())),
                            preferred_element_type=f32)
    cvec[...] = jnp.where(hit > 0, below.astype(i32), -1)

    for l in range(EL):
        for c in weights(l, True):
            c.wait()
        up(l, xgv, pl.ds(0, T), T)

        def down(i, _):
            cols = pl.ds(pl.multiple_of(i * NB, NB), NB)
            t = jnp.dot(hb[...], W2[l, :, cols], preferred_element_type=f32)
            acc[:, cols] = t if l == 0 else acc[:, cols] + t
            return 0

        lax.fori_loop(0, D // NB, down, 0)
        for c in weights(l, False):
            c.start()

    for k in (1, n - 1):
        iy(k).wait_recv()
        ag(k).wait_recv()
        fwd(0 if k == 1 else 1).start()
        fetch(k)
        gather(k)
        for s in range(1, 6):
            xcopy(s, k).start()
    iy(2).wait_recv()
    fwd(0).wait_recv()
    fwd(1).wait_recv()
    fetch(2)
    gather(2)
    for s in range(1, 6):
        xcopy(s, 2).start()
    for s in range(6, G):
        for k in range(1, n):
            xcopy(s, k).start()
    for l in range(EL):
        for c in weights(l, False):
            c.wait()
    for s in range(1, G):
        ixrecv(s).wait_recv()
        gxrecv(s).wait_recv()

    def expert(s):
        @pl.when(s > 0)
        def _():
            for k in range(n):
                xrecv(s, k).wait_recv()
        run([pltpu.make_async_copy(xr.at[s, k, pl.ds(l * C, C)], xb.at[pl.ds(l * RE + k * C, C)],
                                   lsem.at[k * EL + l]) for k in range(n) for l in range(EL)])

        def one(l, _):
            rows = pl.ds(pl.multiple_of(l * RE, 8), RE)
            up(l, xb, rows, RE)

            def down(i, _):
                cols = pl.ds(pl.multiple_of(i * NB, NB), NB)
                eb[rows, cols] = jnp.dot(hb[0:RE, :], W2[l, :, cols], preferred_element_type=f32).astype(bf)
                return 0

            lax.fori_loop(0, D // NB, down, 0)
            return 0

        lax.fori_loop(0, EL, one, 0)
        run([pltpu.make_async_copy(eb.at[pl.ds(l * RE + k * C, C)],
                                   (er.at[s, 0] if k == 0 else es.at[s, k]).at[pl.ds(l * C, C)],
                                   lsem.at[k * EL + l]) for k in range(n) for l in range(EL)])
        for k in range(1, n):
            ecopy(s, k).start()

    def combine(s):
        iv, gv = idxx[s], gx[s]
        r = iota((2 * EG, T), 0)
        oh = one_hot_rows(iv, r + b * EG) & (r < EG)
        mine = [(iv[2 * m:2 * m + 1, :] >= b * EG) & (iv[2 * m:2 * m + 1, :] < b * EG + EG) for m in range(M)]
        hit = mine[0]
        for m in range(1, M):
            hit = hit | mine[m]
        ohf = jnp.where(r == EG, hit.astype(f32), oh.astype(f32))
        cnt = jnp.dot(ohf.astype(bf), tri[...], preferred_element_type=f32).astype(i32)
        slot = jnp.where(hit, cnt[EG:EG + 1, :], -1)
        jd = jnp.zeros((2 * EG, T), i32)
        for q in range(1, n):
            jd = jd + (r >= q * EL).astype(i32)
        kk = jd - j
        kk = jnp.where(kk < 0, kk + n, kk)
        place = kk * CB + (r - jd * EL) * C + cnt
        at = iota((CG, T), 0) == slot
        atb = at.astype(f32).astype(bf)
        for i in range(2):
            ei = jnp.zeros((1, T), i32)
            gi = jnp.zeros((1, T), f32)
            for m in range(M):
                ei = ei + jnp.where(mine[m], iv[2 * m + i:2 * m + i + 1, :], 0)
                gi = gi + jnp.where(mine[m], gv[2 * m + i:2 * m + i + 1, :], 0.0)
            row = jnp.sum(jnp.where((r + b * EG == ei) & (r < EG), place, 0), axis=0, keepdims=True)
            row = jnp.where(hit, row, -1)
            inrow = (iota((R, T), 0) == row).astype(f32).astype(bf)
            putv[i] = lax.dot_general(atb, inrow, (((1,), (1,)), ((), ())), preferred_element_type=f32).astype(bf)
            w = jnp.sum(jnp.where(at, gi, 0.0), axis=1, keepdims=True)
            wqv[i] = jnp.broadcast_to(w, (CG, LANES))
        for k in range(1, n):
            erecv(s, k).wait_recv()
        run([pltpu.make_async_copy(er.at[s, k], rb.at[pl.ds(k * CB, CB)], lsem.at[k]) for k in range(n)])

        def col(i, _):
            cols = pl.ds(pl.multiple_of(i * NB, NB), NB)
            t = jnp.zeros((CG, NB), f32)
            for h in range(2):
                got = jnp.dot(putv[h], rb[:, cols], preferred_element_type=f32)
                t = t + got * jnp.concatenate([wqv[h]] * (NB // LANES), axis=1)
            pb[:, cols] = t.astype(bf)
            return 0

        lax.fori_loop(0, D // NB, col, 0)

        @pl.when(s == 0)
        def _():
            run([pltpu.make_async_copy(pb, pr.at[b], lsem.at[0])])

        @pl.when(s > 0)
        def _():
            run([pltpu.make_async_copy(pb, ps.at[s], lsem.at[0])])
            pcopy(s).start()

    def final(s):
        @pl.when(s > 0)
        def _():
            precv(s).wait_recv()
        g = grp_at(s)
        run([pltpu.make_async_copy(pr.at[g], fb, lsem.at[0])])
        code = jnp.sum(jnp.where(iota((T, LANES), 1) == g, cvec[...], 0), axis=1, keepdims=True)
        at = (iota((T, CG), 1) == code).astype(f32).astype(bf)

        def col(i, _):
            cols = pl.ds(pl.multiple_of(i * NB, NB), NB)
            acc[:, cols] = acc[:, cols] + jnp.dot(at, fb[:, cols], preferred_element_type=f32)
            return 0

        lax.fori_loop(0, D // NB, col, 0)

    def step(s, _):
        @pl.when(s < G)
        def _():
            expert(s)

        @pl.when((s > 0) & (s <= G))
        def _():
            combine(s - 1)

        @pl.when(s >= LAG)
        def _():
            final(s - LAG)
        return 0

    lax.fori_loop(0, G + LAG, step, 0)

    def out(i, _):
        cols = pl.ds(pl.multiple_of(i * NB, NB), NB)
        xgv[:, cols] = acc[:, cols].astype(bf)
        return 0

    lax.fori_loop(0, D // NB, out, 0)
    run([pltpu.make_async_copy(xgv, y_ref, lsem.at[0])])

    for k in range(1, n):
        iy(k).wait_send()
    ag(1).wait_send()
    ag(n - 1).wait_send()
    fwd(0).wait_send()
    fwd(1).wait_send()
    for s in range(1, G):
        ix(s).wait_send()
        gxc(s).wait_send()
        for k in range(n):
            xcopy(s, k).wait_send()
        pcopy(s).wait_send()
    for s in range(G):
        for k in range(1, n):
            ecopy(s, k).wait_send()


def solution(mesh):
    G = mesh.shape['grp']
    n = mesh.shape['ing']
    tok = P(('dp', 'grp', 'ing'), None)
    tok3 = P(('dp', 'grp', 'ing'), None, None)
    exp = P(('grp', 'ing'), None, None)

    def local(x, idx, g, w1, w3, w2, s1, s3, s2):
        T, D = x.shape
        _, M, KG = idx.shape
        K = M * KG
        EL, _, F = w1.shape
        E = EL * G * n
        C = (3 * T * K + 2 * E - 1) // (2 * E)
        CG = min(T, 3 * T * M // (2 * G))
        CB = EL * C
        R = n * CB
        flat = idx.reshape(T, K)
        it = jnp.pad(flat.T, ((0, 8 - K), (0, 0)))
        gt = jnp.pad(g.reshape(T, K).T, ((0, 8 - K), (0, 0)))
        ic = jnp.pad(flat, ((0, 0), (0, LANES - K)))
        anyspec = pl.BlockSpec(memory_space=pl.ANY)
        bf, f32, i32 = jnp.bfloat16, jnp.float32, jnp.int32
        sds = jax.ShapeDtypeStruct
        dma = lambda *s: pltpu.SemaphoreType.DMA(s)
        out = pl.pallas_call(
            functools.partial(_moe_kernel, G, n, EL, C, CG, T, D, F, K),
            out_shape=[sds((T, D), bf), sds((G, CG, D), bf), sds((n, T, D), bf), sds((n, G, CB, D), bf),
                       sds((G, n, CB, D), bf), sds((G, n, CB, D), bf), sds((G, n, CB, D), bf),
                       sds((G, CG, D), bf)],
            in_specs=[anyspec] * 10,
            out_specs=[anyspec] * 8,
            scratch_shapes=[
                pltpu.VMEM((EL, D, F), bf), pltpu.VMEM((EL, D, F), bf), pltpu.VMEM((EL, F, D), bf),
                pltpu.VMEM((G * CB, D), bf), pltpu.VMEM((R, D), bf), pltpu.VMEM((R, D), bf),
                pltpu.VMEM((CG, D), bf), pltpu.VMEM((CG, D), bf), pltpu.VMEM((T, F), bf),
                pltpu.VMEM((T, D), bf), pltpu.VMEM((G * CB, T), bf),
                pltpu.VMEM((KG, CG, R), bf), pltpu.VMEM((KG, CG, LANES), f32),
                pltpu.VMEM((T, D), f32), pltpu.VMEM((T, T), bf), pltpu.VMEM((T, LANES), i32),
                pltpu.VMEM((T, LANES), i32), pltpu.VMEM((n, 8, T), i32), pltpu.VMEM((G, 8, T), i32),
                pltpu.VMEM((G, 8, T), f32),
                dma(n), dma(n), dma(n), dma(n), dma(G), dma(G), dma(G), dma(G),
                dma(G, n), dma(G, n), dma(G, n), dma(G, n), dma(G), dma(G), dma(G + n), dma(EL, 3),
            ],
            compiler_params=pltpu.CompilerParams(
                collective_id=0, has_side_effects=True, vmem_limit_bytes=63 * 1024 * 1024),
            name="moe",
        )(x, it, gt, ic, w1, w3, w2, s1, s3, s2)
        return out[0]

    return jax.shard_map(local, mesh=mesh, in_specs=(tok, tok3, tok3, exp, exp, exp, P(), P(), P()),
                         out_specs=tok, check_vma=False)
```

```python
import functools

import jax
import jax.numpy as jnp
from jax import lax
from jax.experimental import pallas as pl
from jax.experimental.pallas import tpu as pltpu
from jax.sharding import PartitionSpec as P

MESH = pl.DeviceIdType.MESH
LANES = 128


def _moe_kernel(G, n, EL, C, CG, T, D, F, K,
                x_ref, it_ref, gt_ref, w1_ref, w3_ref, w2_ref, s1_ref, s3_ref, s2_ref,
                y_ref, pr, xg, xs, xr, er, ps,
                W1, W3, W2, xb, eb, rb, pb, fb, hb, xgv, selv, putv, wqv, acc, tri, cvec,
                idxy, idxx, gx,
                agS, agR, iyS, iyR, ixS, ixR, gxS, gxR, xS, xR, eS, eR, pS, pR, oS, lsem, wsem, fsem):
    EG = EL * n
    CB = EL * C
    R = n * CB
    RE = n * C
    M = K // 2
    H = T // 2
    NB = min(256, D)
    LAG = 5
    SELF = G - 1
    bf = jnp.bfloat16
    f32 = jnp.float32
    i32 = jnp.int32
    d = lax.axis_index('dp')
    j = lax.axis_index('ing')
    b = lax.axis_index('grp')
    chips = G // 2
    chip, core = b // 2, b % 2

    def grp_at(s):
        t = s - (s // 4) * (2 * s - 7)
        dc = (t * (t + 1) // 2) % 4
        dcore = (s // 4 + 1 - (s % 7 + 6) // 7) % 2
        return 2 * ((chip + dc) % chips) + (core + dcore) % 2

    def inv(s):
        u = s % 4
        return s + (((u + 1) // 2) % 2) * (3 - 2 * u)

    def xdev(s):
        return (d, j, grp_at(s))

    def ydev(k):
        return (d, (j + k) % n, b)

    def iota(shape, dim):
        return lax.broadcasted_iota(i32, shape, dim)

    def remote(src, dst, ss, rs, dev):
        return pltpu.make_async_remote_copy(src_ref=src, dst_ref=dst, send_sem=ss, recv_sem=rs,
                                            device_id=dev, device_id_type=MESH)

    barrier = pltpu.get_barrier_semaphore()
    for k in range(1, n):
        pl.semaphore_signal(barrier, 1, device_id=ydev(k), device_id_type=MESH)
    for s in range(SELF):
        pl.semaphore_signal(barrier, 1, device_id=xdev(s), device_id_type=MESH)
    pl.semaphore_wait(barrier, n - 1 + G - 1)

    def ag(k):
        return remote(x_ref, xg.at[k], agS.at[k], agR.at[k], ydev(n - k))

    def fwd(h):
        k, dev = (1, n - 1) if h == 0 else (n - 1, 1)
        rows = pl.ds(h * H, H)
        return remote(xg.at[k, rows], xg.at[2, rows], agS.at[2 * h], agR.at[2 * h], ydev(dev))

    def iy(k):
        return remote(it_ref, idxy.at[k], iyS.at[k], iyR.at[k], ydev(n - k))

    def ix(s):
        return remote(it_ref, idxx.at[inv(s)], ixS.at[s], ixR.at[inv(s)], xdev(s))

    def ixrecv(s):
        return remote(it_ref, idxx.at[s], ixS.at[s], ixR.at[s], xdev(s))

    def gxc(s):
        return remote(gt_ref, gx.at[inv(s)], gxS.at[s], gxR.at[inv(s)], xdev(s))

    def gxrecv(s):
        return remote(gt_ref, gx.at[s], gxS.at[s], gxR.at[s], xdev(s))

    def xcopy(s, k):
        return remote(xs.at[k, grp_at(s)], xr.at[inv(s), k], xS.at[s, k], xR.at[inv(s), k], xdev(s))

    def xrecv(s, k):
        return remote(xs.at[k, grp_at(s)], xr.at[s, k], xS.at[s, k], xR.at[s, k], xdev(s))

    def erows(l, k):
        return pl.ds(pl.multiple_of(l * RE + k * C, 8), C)

    def lrows(l):
        return pl.ds(pl.multiple_of(l * C, 8), C)

    def ecopy(s, k, l):
        return remote(eb.at[s % 2, erows(l, k)], er.at[s, n - k, lrows(l)],
                      eS.at[s, l * n + k], eR.at[s, l * n + n - k], ydev(k))

    def erecv(s, k, l):
        return remote(eb.at[s % 2, erows(l, k)], er.at[s, k, lrows(l)],
                      eS.at[s, l * n + k], eR.at[s, l * n + k], ydev(k))

    def eown(s, l):
        return pltpu.make_async_copy(eb.at[s % 2, erows(l, 0)], er.at[s, 0, lrows(l)], oS.at[s, l])

    def pcopy(s):
        return remote(ps.at[s], pr.at[b], pS.at[s], pR.at[b], xdev(s))

    def precv(s):
        g = grp_at(s)
        return remote(ps.at[s], pr.at[g], pS.at[s], pR.at[g], xdev(s))

    def run(copies):
        for c in copies:
            c.start()
        for c in copies:
            c.wait()

    for k in range(1, n):
        iy(k).start()
    ag(1).start()
    ag(n - 1).start()

    def weights(l, shared):
        cols = pl.ds(l * F, F)
        srcs = ((s1_ref.at[:, cols], s3_ref.at[:, cols], s2_ref.at[cols]) if shared
                else (w1_ref.at[l], w3_ref.at[l], w2_ref.at[l]))
        return [pltpu.make_async_copy(s, w.at[l], wsem.at[l, i])
                for i, (s, w) in enumerate(zip(srcs, (W1, W3, W2)))]

    run([pltpu.make_async_copy(it_ref, idxy.at[0], lsem.at[0]),
         pltpu.make_async_copy(it_ref, idxx.at[SELF], lsem.at[1]),
         pltpu.make_async_copy(gt_ref, gx.at[SELF], lsem.at[2]),
         pltpu.make_async_copy(x_ref, xgv, lsem.at[4])])
    for s in range(SELF):
        ix(s).start()
        gxc(s).start()
    for l in range(EL):
        for c in weights(l, True):
            c.start()
    tri[...] = (iota((T, T), 0) < iota((T, T), 1)).astype(f32).astype(bf)

    def one_hot_rows(iv, eid):
        oh = iv[0:1, :] == eid
        for i in range(1, K):
            oh = oh | (iv[i:i + 1, :] == eid)
        return oh

    def gather(k):
        iv = idxy[k]
        r = iota((G * EL, T), 0)
        g_of = jnp.zeros((G * EL, T), i32)
        for q in range(1, G):
            g_of = g_of + (r >= q * EL).astype(i32)
        eid = g_of * (EG - EL) + r + j * EL
        oh = one_hot_rows(iv, eid)
        rank = jnp.dot(oh.astype(f32).astype(bf), tri[...], preferred_element_type=f32)
        code = jnp.where(oh, rank.astype(i32), -(EL * C))
        row = iota((CB, T), 0)
        for g in range(G):
            want = code[g * EL:g * EL + 1, :]
            for l in range(1, EL):
                want = jnp.where(row < l * C, want, code[g * EL + l:g * EL + l + 1, :] + l * C)
            selv[g * CB:(g + 1) * CB, :] = (row == want).astype(f32).astype(bf)

        def col(i, _):
            cols = pl.ds(pl.multiple_of(i * NB, NB), NB)
            xb[:, cols] = jnp.dot(selv[...], xgv[:, cols], preferred_element_type=f32).astype(bf)
            return 0

        lax.fori_loop(0, D // NB, col, 0)
        run([pltpu.make_async_copy(xb.at[pl.ds(g * CB, CB)], xs.at[k, g], lsem.at[g]) for g in range(G)]
            + [pltpu.make_async_copy(xb.at[pl.ds(pl.multiple_of(b * CB, 8), CB)], xr.at[SELF, k], lsem.at[G])])

    def fetch(k):
        run([pltpu.make_async_copy(xg.at[k], xgv, lsem.at[0])])

    def up(l, src, rows, m):
        def body(i, _):
            cols = pl.ds(pl.multiple_of(i * LANES, LANES), LANES)
            w = jnp.concatenate([W1[l, :, cols], W3[l, :, cols]], axis=1)
            hh = jnp.dot(src[rows, :], w, preferred_element_type=f32)
            a, c = hh[:, :LANES], hh[:, LANES:]
            hb[0:m, cols] = (a * jax.nn.sigmoid(a) * c).astype(bf)
            return 0

        lax.fori_loop(0, F // LANES, body, 0)

    gather(0)
    for s in (1, 2, 5, 6, 3, 4, 0):
        xcopy(s, 0).start()

    iv = idxy[0]
    gid = iota((2 * G, T), 0) * EG
    hit = jnp.zeros((2 * G, T), i32)
    for m in range(M):
        v = iv[2 * m:2 * m + 1, :]
        hit = hit + ((v >= gid) & (v < gid + EG)).astype(i32)
    below = jnp.dot(hit.astype(f32).astype(bf), tri[...], preferred_element_type=f32)
    code = jnp.where(hit > 0, below, -1.0)
    cvec[...] = jnp.concatenate([code, jnp.zeros((LANES - 2 * G, T), f32)], axis=0).T

    for l in range(EL):
        for c in weights(l, True):
            c.wait()
        up(l, xgv, pl.ds(0, T), T)

        def down(i, _):
            cols = pl.ds(pl.multiple_of(i * NB, NB), NB)
            t = jnp.dot(hb[...], W2[l, :, cols], preferred_element_type=f32)
            acc[:, cols] = t if l == 0 else acc[:, cols] + t
            return 0

        lax.fori_loop(0, D // NB, down, 0)
        for c in weights(l, False):
            c.start()

    for k in (1, n - 1):
        iy(k).wait_recv()
        ag(k).wait_recv()
        fwd(0 if k == 1 else 1).start()
        fetch(k)
        gather(k)
        for s in range(3):
            xcopy(s, k).start()
    iy(2).wait_recv()
    fwd(0).wait_recv()
    fwd(1).wait_recv()
    fetch(2)
    gather(2)
    for s in range(3):
        xcopy(s, 2).start()
    for s in range(3, SELF):
        for k in range(1, n):
            xcopy(s, k).start()
    for l in range(EL):
        for c in weights(l, False):
            c.wait()
    for s in range(SELF):
        ixrecv(s).wait_recv()
        gxrecv(s).wait_recv()

    def expert(s):
        @pl.when(s < SELF)
        def _():
            for k in range(n):
                xrecv(s, k).wait_recv()

        def load(l, k):
            return pltpu.make_async_copy(xr.at[s, k, lrows(l)], xb.at[erows(l, k)], lsem.at[l * n + k])

        for l in range(EL):
            for k in range(n):
                load(l, k).start()

        @pl.when(s >= 2)
        def _():
            for l in range(EL):
                for k in range(1, n):
                    ecopy(s - 2, k, l).wait_send()

        def one(l, _):
            for k in range(n):
                load(l, k).wait()
            rows = pl.ds(pl.multiple_of(l * RE, 8), RE)
            up(l, xb, rows, RE)

            def down(i, _):
                cols = pl.ds(pl.multiple_of(i * NB, NB), NB)
                eb[s % 2, rows, cols] = jnp.dot(hb[0:RE, :], W2[l, :, cols], preferred_element_type=f32).astype(bf)
                return 0

            lax.fori_loop(0, D // NB, down, 0)
            for k in (1, n - 1, 2):
                ecopy(s, k, l).start()
            eown(s, l).start()
            return 0

        lax.fori_loop(0, EL, one, 0)

    def combine(s):
        iv, gv = idxx[s], gx[s]
        r = iota((2 * EG, T), 0)
        oh = one_hot_rows(iv, r + b * EG) & (r < EG)
        mine = [(iv[2 * m:2 * m + 1, :] >= b * EG) & (iv[2 * m:2 * m + 1, :] < b * EG + EG) for m in range(M)]
        hit = mine[0]
        for m in range(1, M):
            hit = hit | mine[m]
        ohf = jnp.where(r == EG, hit.astype(f32), oh.astype(f32))
        cnt = jnp.dot(ohf.astype(bf), tri[...], preferred_element_type=f32).astype(i32)
        slot = jnp.where(hit, cnt[EG:EG + 1, :], -1)
        jd = jnp.zeros((2 * EG, T), i32)
        for q in range(1, n):
            jd = jd + (r >= q * EL).astype(i32)
        kk = jd - j
        kk = jnp.where(kk < 0, kk + n, kk)
        place = kk * CB + (r - jd * EL) * C + cnt
        at = iota((CG, T), 0) == slot
        atb = at.astype(f32).astype(bf)
        for i in range(2):
            ei = jnp.zeros((1, T), i32)
            gi = jnp.zeros((1, T), f32)
            for m in range(M):
                ei = ei + jnp.where(mine[m], iv[2 * m + i:2 * m + i + 1, :], 0)
                gi = gi + jnp.where(mine[m], gv[2 * m + i:2 * m + i + 1, :], 0.0)
            row = jnp.sum(jnp.where((r + b * EG == ei) & (r < EG), place, 0), axis=0, keepdims=True)
            row = jnp.where(hit, row, -1)
            inrow = (iota((R, T), 0) == row).astype(f32).astype(bf)
            putv[i] = lax.dot_general(atb, inrow, (((1,), (1,)), ((), ())), preferred_element_type=f32).astype(bf)
            w = jnp.sum(jnp.where(at, gi, 0.0), axis=1, keepdims=True)
            wqv[i] = jnp.broadcast_to(w, (CG, LANES))
        loads = [pltpu.make_async_copy(er.at[s, k], rb.at[pl.ds(k * CB, CB)], lsem.at[k]) for k in range(n)]
        for l in range(EL):
            eown(s, l).wait()
        loads[0].start()
        for k in (1, n - 1, 2):
            for l in range(EL):
                erecv(s, k, l).wait_recv()
            loads[k].start()
        for c in loads:
            c.wait()

        def col(i, _):
            cols = pl.ds(pl.multiple_of(i * NB, NB), NB)
            t = jnp.zeros((CG, NB), f32)
            for h in range(2):
                got = jnp.dot(putv[h], rb[:, cols], preferred_element_type=f32)
                t = t + got * jnp.concatenate([wqv[h]] * (NB // LANES), axis=1)
            pb[:, cols] = t.astype(bf)
            return 0

        lax.fori_loop(0, D // NB, col, 0)

        @pl.when(s == SELF)
        def _():
            pltpu.make_async_copy(pb, pr.at[b], lsem.at[0]).start()

        @pl.when(s < SELF)
        def _():
            pltpu.make_async_copy(pb, ps.at[s], lsem.at[0]).start()

    def send_back(s):
        pltpu.make_async_copy(pb, ps.at[s], lsem.at[0]).wait()

        @pl.when(s < SELF)
        def _():
            pcopy(s).start()

    def final_load(s):
        @pl.when(s < SELF)
        def _():
            precv(s).wait_recv()
        pltpu.make_async_copy(pr.at[grp_at(s)], fb, fsem.at[0]).start()

    def final(s):
        g = grp_at(s)
        pltpu.make_async_copy(pr.at[g], fb, fsem.at[0]).wait()
        code = jnp.sum(jnp.where(iota((T, LANES), 1) == g, cvec[...], 0.0), axis=1, keepdims=True)
        at = (iota((T, CG), 1) == code.astype(i32)).astype(f32).astype(bf)

        def col(i, _):
            cols = pl.ds(pl.multiple_of(i * NB, NB), NB)
            acc[:, cols] = acc[:, cols] + jnp.dot(at, fb[:, cols], preferred_element_type=f32)
            return 0

        lax.fori_loop(0, D // NB, col, 0)

    def step(s, _):
        @pl.when(s < G)
        def _():
            expert(s)

        @pl.when((s > 0) & (s <= G))
        def _():
            combine(s - 1)

        @pl.when(s >= LAG)
        def _():
            final_load(s - LAG)

        @pl.when((s > 0) & (s <= G))
        def _():
            send_back(s - 1)

        @pl.when(s >= LAG)
        def _():
            final(s - LAG)
        return 0

    lax.fori_loop(0, G + LAG, step, 0)

    def out(i, _):
        cols = pl.ds(pl.multiple_of(i * NB, NB), NB)
        xgv[:, cols] = acc[:, cols].astype(bf)
        return 0

    lax.fori_loop(0, D // NB, out, 0)
    run([pltpu.make_async_copy(xgv, y_ref, lsem.at[0])])

    for k in range(1, n):
        iy(k).wait_send()
    ag(1).wait_send()
    ag(n - 1).wait_send()
    fwd(0).wait_send()
    fwd(1).wait_send()
    for s in range(SELF):
        ix(s).wait_send()
        gxc(s).wait_send()
        for k in range(n):
            xcopy(s, k).wait_send()
        pcopy(s).wait_send()
    for s in range(G - 2, G):
        for l in range(EL):
            for k in range(1, n):
                ecopy(s, k, l).wait_send()


def solution(mesh):
    G = mesh.shape['grp']
    n = mesh.shape['ing']
    tok = P(('dp', 'grp', 'ing'), None)
    tok3 = P(('dp', 'grp', 'ing'), None, None)
    exp = P(('grp', 'ing'), None, None)

    def local(x, idx, g, w1, w3, w2, s1, s3, s2):
        T, D = x.shape
        _, M, KG = idx.shape
        K = M * KG
        EL, _, F = w1.shape
        E = EL * G * n
        C = (3 * T * K + 2 * E - 1) // (2 * E)
        CG = min(T, 3 * T * M // (2 * G))
        CB = EL * C
        R = n * CB
        flat = idx.reshape(T, K)
        it = flat.T
        gt = g.reshape(T, K).T
        anyspec = pl.BlockSpec(memory_space=pl.ANY)
        bf, f32, i32 = jnp.bfloat16, jnp.float32, jnp.int32
        sds = jax.ShapeDtypeStruct
        dma = lambda *s: pltpu.SemaphoreType.DMA(s)
        out = pl.pallas_call(
            functools.partial(_moe_kernel, G, n, EL, C, CG, T, D, F, K),
            out_shape=[sds((T, D), bf), sds((G, CG, D), bf), sds((n, T, D), bf), sds((n, G, CB, D), bf),
                       sds((G, n, CB, D), bf), sds((G, n, CB, D), bf),
                       sds((G, CG, D), bf)],
            in_specs=[anyspec] * 9,
            out_specs=[anyspec] * 7,
            scratch_shapes=[
                pltpu.VMEM((EL, D, F), bf), pltpu.VMEM((EL, D, F), bf), pltpu.VMEM((EL, F, D), bf),
                pltpu.VMEM((G * CB, D), bf), pltpu.VMEM((2, R, D), bf), pltpu.VMEM((R, D), bf),
                pltpu.VMEM((CG, D), bf), pltpu.VMEM((CG, D), bf), pltpu.VMEM((T, F), bf),
                pltpu.VMEM((T, D), bf), pltpu.VMEM((G * CB, T), bf),
                pltpu.VMEM((KG, CG, R), bf), pltpu.VMEM((KG, CG, LANES), f32),
                pltpu.VMEM((T, D), f32), pltpu.VMEM((T, T), bf), pltpu.VMEM((T, LANES), f32),
                pltpu.VMEM((n, K, T), i32), pltpu.VMEM((G, K, T), i32), pltpu.VMEM((G, K, T), f32),
                dma(n), dma(n), dma(n), dma(n), dma(G), dma(G), dma(G), dma(G),
                dma(G, n), dma(G, n), dma(G, EL * n), dma(G, EL * n), dma(G), dma(G), dma(G, EL),
                dma(G + n), dma(EL, 3), dma(1),
            ],
            compiler_params=pltpu.CompilerParams(
                collective_id=0, has_side_effects=True, vmem_limit_bytes=63 * 1024 * 1024),
            name="moe",
        )(x, it, gt, w1, w3, w2, s1, s3, s2)
        return out[0]

    return jax.shard_map(local, mesh=mesh, in_specs=(tok, tok3, tok3, exp, exp, exp, P(), P(), P()),
                         out_specs=tok, check_vma=False)
```

```python
import functools

import jax
import jax.numpy as jnp
from jax import lax
from jax.experimental import pallas as pl
from jax.experimental.pallas import tpu as pltpu
from jax.sharding import PartitionSpec as P

MESH = pl.DeviceIdType.MESH
LANES = 128


def _moe_kernel(G, n, EL, C, CG, T, D, F, K,
                x_ref, it_ref, gt_ref, w1_ref, w3_ref, w2_ref, s1_ref, s3_ref, s2_ref,
                y_ref, pr, xg, xs, xr, er, ps,
                W1, W3, W2, xb, eb, rb, pb, fb, hb, xgv, selv, putv, wqv, acc, tri, cvec,
                idxy, idxx, gx,
                agS, agR, iyS, iyR, ixS, ixR, gxS, gxR, xS, xR, eS, eR, pS, pR, oS, lsem, wsem, fsem):
    EG = EL * n
    CB = EL * C
    R = n * CB
    RE = n * C
    M = K // 2
    H = T // 2
    NB = min(512, D)
    LAG = 5
    SELF = G - 1
    bf = jnp.bfloat16
    f32 = jnp.float32
    i32 = jnp.int32
    d = lax.axis_index('dp')
    j = lax.axis_index('ing')
    b = lax.axis_index('grp')
    chips = G // 2
    chip, core = b // 2, b % 2

    def grp_at(s):
        t = s - (s // 4) * (2 * s - 7)
        dc = (t * (t + 1) // 2) % 4
        dcore = (s // 4 + 1 - (s % 7 + 6) // 7) % 2
        return 2 * ((chip + dc) % chips) + (core + dcore) % 2

    def inv(s):
        u = s % 4
        return s + (((u + 1) // 2) % 2) * (3 - 2 * u)

    def xdev(s):
        return (d, j, grp_at(s))

    def ydev(k):
        return (d, (j + k) % n, b)

    def iota(shape, dim):
        return lax.broadcasted_iota(i32, shape, dim)

    def remote(src, dst, ss, rs, dev):
        return pltpu.make_async_remote_copy(src_ref=src, dst_ref=dst, send_sem=ss, recv_sem=rs,
                                            device_id=dev, device_id_type=MESH)

    barrier = pltpu.get_barrier_semaphore()
    for k in range(1, n):
        pl.semaphore_signal(barrier, 1, device_id=ydev(k), device_id_type=MESH)
    for s in range(SELF):
        pl.semaphore_signal(barrier, 1, device_id=xdev(s), device_id_type=MESH)
    pl.semaphore_wait(barrier, n - 1 + G - 1)

    def ag(k):
        return remote(x_ref, xg.at[k], agS.at[k], agR.at[k], ydev(n - k))

    def fwd(h):
        k, dev = (1, n - 1) if h == 0 else (n - 1, 1)
        rows = pl.ds(h * H, H)
        return remote(xg.at[k, rows], xg.at[2, rows], agS.at[2 * h], agR.at[2 * h], ydev(dev))

    def iy(k):
        return remote(it_ref, idxy.at[k], iyS.at[k], iyR.at[k], ydev(n - k))

    def ix(s):
        return remote(it_ref, idxx.at[inv(s)], ixS.at[s], ixR.at[inv(s)], xdev(s))

    def ixrecv(s):
        return remote(it_ref, idxx.at[s], ixS.at[s], ixR.at[s], xdev(s))

    def gxc(s):
        return remote(gt_ref, gx.at[inv(s)], gxS.at[s], gxR.at[inv(s)], xdev(s))

    def gxrecv(s):
        return remote(gt_ref, gx.at[s], gxS.at[s], gxR.at[s], xdev(s))

    def xcopy(s, k):
        return remote(xs.at[k, grp_at(s)], xr.at[inv(s), k], xS.at[s, k], xR.at[inv(s), k], xdev(s))

    def xrecv(s, k):
        return remote(xs.at[k, grp_at(s)], xr.at[s, k], xS.at[s, k], xR.at[s, k], xdev(s))

    def erows(l, k):
        return pl.ds(pl.multiple_of(l * RE + k * C, 8), C)

    def lrows(l):
        return pl.ds(pl.multiple_of(l * C, 8), C)

    def ecopy(s, k, l):
        return remote(eb.at[s % 2, erows(l, k)], er.at[s, n - k, lrows(l)],
                      eS.at[s, l * n + k], eR.at[s, l * n + n - k], ydev(k))

    def erecv(s, k, l):
        return remote(eb.at[s % 2, erows(l, k)], er.at[s, k, lrows(l)],
                      eS.at[s, l * n + k], eR.at[s, l * n + k], ydev(k))

    def eown(s, l):
        return pltpu.make_async_copy(eb.at[s % 2, erows(l, 0)], er.at[s, 0, lrows(l)], oS.at[s, l])

    def pcopy(s):
        return remote(ps.at[s], pr.at[b], pS.at[s], pR.at[b], xdev(s))

    def precv(s):
        g = grp_at(s)
        return remote(ps.at[s], pr.at[g], pS.at[s], pR.at[g], xdev(s))

    def run(copies):
        for c in copies:
            c.start()
        for c in copies:
            c.wait()

    for k in range(1, n):
        iy(k).start()
    ag(1).start()
    ag(n - 1).start()

    def weights(l, shared):
        cols = pl.ds(l * F, F)
        srcs = ((s1_ref.at[:, cols], s3_ref.at[:, cols], s2_ref.at[cols]) if shared
                else (w1_ref.at[l], w3_ref.at[l], w2_ref.at[l]))
        return [pltpu.make_async_copy(s, w.at[l], wsem.at[l, i])
                for i, (s, w) in enumerate(zip(srcs, (W1, W3, W2)))]

    run([pltpu.make_async_copy(it_ref, idxy.at[0], lsem.at[0]),
         pltpu.make_async_copy(it_ref, idxx.at[SELF], lsem.at[1]),
         pltpu.make_async_copy(gt_ref, gx.at[SELF], lsem.at[2]),
         pltpu.make_async_copy(x_ref, xgv, lsem.at[4])])
    for s in range(SELF):
        ix(s).start()
        gxc(s).start()
    for l in range(EL):
        for c in weights(l, True):
            c.start()
    tri[...] = (iota((T, T), 0) < iota((T, T), 1)).astype(f32).astype(bf)

    def one_hot_rows(iv, eid):
        oh = iv[0:1, :] == eid
        for i in range(1, K):
            oh = oh | (iv[i:i + 1, :] == eid)
        return oh

    def gather(k):
        iv = idxy[k]
        r = iota((G * EL, T), 0)
        g_of = jnp.zeros((G * EL, T), i32)
        for q in range(1, G):
            g_of = g_of + (r >= q * EL).astype(i32)
        eid = g_of * (EG - EL) + r + j * EL
        oh = one_hot_rows(iv, eid)
        rank = jnp.dot(oh.astype(f32).astype(bf), tri[...], preferred_element_type=f32)
        code = jnp.where(oh, rank.astype(i32), -(EL * C))
        row = iota((CB, T), 0)
        for g in range(G):
            want = code[g * EL:g * EL + 1, :]
            for l in range(1, EL):
                want = jnp.where(row < l * C, want, code[g * EL + l:g * EL + l + 1, :] + l * C)
            selv[g * CB:(g + 1) * CB, :] = (row == want).astype(f32).astype(bf)

        def col(i, _):
            cols = pl.ds(pl.multiple_of(i * NB, NB), NB)
            xb[:, cols] = jnp.dot(selv[...], xgv[:, cols], preferred_element_type=f32).astype(bf)
            return 0

        lax.fori_loop(0, D // NB, col, 0, unroll=True)
        run([pltpu.make_async_copy(xb.at[pl.ds(g * CB, CB)], xs.at[k, g], lsem.at[g]) for g in range(G)]
            + [pltpu.make_async_copy(xb.at[pl.ds(pl.multiple_of(b * CB, 8), CB)], xr.at[SELF, k], lsem.at[G])])

    def fetch(k):
        run([pltpu.make_async_copy(xg.at[k], xgv, lsem.at[0])])

    def up(l, src, rows, m):
        def body(i, _):
            cols = pl.ds(pl.multiple_of(i * LANES, LANES), LANES)
            w = jnp.concatenate([W1[l, :, cols], W3[l, :, cols]], axis=1)
            hh = jnp.dot(src[rows, :], w, preferred_element_type=f32)
            a, c = hh[:, :LANES], hh[:, LANES:]
            hb[0:m, cols] = (a * jax.nn.sigmoid(a) * c).astype(bf)
            return 0

        lax.fori_loop(0, F // LANES, body, 0, unroll=True)

    gather(0)
    for s in (1, 2, 5, 6, 3, 4, 0):
        xcopy(s, 0).start()

    iv = idxy[0]
    gid = iota((2 * G, T), 0) * EG
    hit = jnp.zeros((2 * G, T), i32)
    for m in range(M):
        v = iv[2 * m:2 * m + 1, :]
        hit = hit + ((v >= gid) & (v < gid + EG)).astype(i32)
    below = jnp.dot(hit.astype(f32).astype(bf), tri[...], preferred_element_type=f32)
    code = jnp.where(hit > 0, below, -1.0)
    cvec[...] = jnp.concatenate([code, jnp.zeros((LANES - 2 * G, T), f32)], axis=0).T

    for l in range(EL):
        for c in weights(l, True):
            c.wait()
        up(l, xgv, pl.ds(0, T), T)

        def down(i, _):
            cols = pl.ds(pl.multiple_of(i * NB, NB), NB)
            t = jnp.dot(hb[...], W2[l, :, cols], preferred_element_type=f32)
            acc[:, cols] = t if l == 0 else acc[:, cols] + t
            return 0

        lax.fori_loop(0, D // NB, down, 0, unroll=True)
        for c in weights(l, False):
            c.start()

    for k in (1, n - 1):
        iy(k).wait_recv()
        ag(k).wait_recv()
        fwd(0 if k == 1 else 1).start()
        fetch(k)
        gather(k)
        for s in (0, 1, 2, 3):
            xcopy(s, k).start()
    iy(2).wait_recv()
    fwd(0).wait_recv()
    fwd(1).wait_recv()
    fetch(2)
    gather(2)
    for s in range(4):
        xcopy(s, 2).start()
    for s in range(4, SELF):
        for k in range(1, n):
            xcopy(s, k).start()
    for l in range(EL):
        for c in weights(l, False):
            c.wait()
    for s in range(SELF):
        ixrecv(s).wait_recv()
        gxrecv(s).wait_recv()

    def expert(s):
        @pl.when(s < SELF)
        def _():
            for k in range(n):
                xrecv(s, k).wait_recv()

        def load(l, k):
            return pltpu.make_async_copy(xr.at[s, k, lrows(l)], xb.at[erows(l, k)], lsem.at[l * n + k])

        for l in range(EL):
            for k in range(n):
                load(l, k).start()

        @pl.when(s >= 2)
        def _():
            for l in range(EL):
                for k in range(1, n):
                    ecopy(s - 2, k, l).wait_send()

        def one(l, _):
            for k in range(n):
                load(l, k).wait()
            rows = pl.ds(pl.multiple_of(l * RE, 8), RE)
            up(l, xb, rows, RE)

            def down(i, _):
                cols = pl.ds(pl.multiple_of(i * NB, NB), NB)
                eb[s % 2, rows, cols] = jnp.dot(hb[0:RE, :], W2[l, :, cols], preferred_element_type=f32).astype(bf)
                return 0

            lax.fori_loop(0, D // NB, down, 0, unroll=True)
            for k in (1, n - 1, 2):
                ecopy(s, k, l).start()
            eown(s, l).start()
            return 0

        lax.fori_loop(0, EL, one, 0)

    def combine(s):
        iv, gv = idxx[s], gx[s]
        r = iota((2 * EG, T), 0)
        oh = one_hot_rows(iv, r + b * EG) & (r < EG)
        mine = [(iv[2 * m:2 * m + 1, :] >= b * EG) & (iv[2 * m:2 * m + 1, :] < b * EG + EG) for m in range(M)]
        hit = mine[0]
        for m in range(1, M):
            hit = hit | mine[m]
        ohf = jnp.where(r == EG, hit.astype(f32), oh.astype(f32))
        cnt = jnp.dot(ohf.astype(bf), tri[...], preferred_element_type=f32).astype(i32)
        slot = jnp.where(hit, cnt[EG:EG + 1, :], -1)
        jd = jnp.zeros((2 * EG, T), i32)
        for q in range(1, n):
            jd = jd + (r >= q * EL).astype(i32)
        kk = jd - j
        kk = jnp.where(kk < 0, kk + n, kk)
        place = kk * CB + (r - jd * EL) * C + cnt
        at = iota((CG, T), 0) == slot
        atb = at.astype(f32).astype(bf)
        for i in range(2):
            ei = jnp.zeros((1, T), i32)
            gi = jnp.zeros((1, T), f32)
            for m in range(M):
                ei = ei + jnp.where(mine[m], iv[2 * m + i:2 * m + i + 1, :], 0)
                gi = gi + jnp.where(mine[m], gv[2 * m + i:2 * m + i + 1, :], 0.0)
            row = jnp.sum(jnp.where((r + b * EG == ei) & (r < EG), place, 0), axis=0, keepdims=True)
            row = jnp.where(hit, row, -1)
            inrow = (iota((R, T), 0) == row).astype(f32).astype(bf)
            putv[i] = lax.dot_general(atb, inrow, (((1,), (1,)), ((), ())), preferred_element_type=f32).astype(bf)
            w = jnp.sum(jnp.where(at, gi, 0.0), axis=1, keepdims=True)
            wqv[i] = jnp.broadcast_to(w, (CG, LANES))
        loads = [pltpu.make_async_copy(er.at[s, k], rb.at[pl.ds(k * CB, CB)], lsem.at[k]) for k in range(n)]
        for l in range(EL):
            eown(s, l).wait()
        loads[0].start()
        for k in (1, n - 1, 2):
            for l in range(EL):
                erecv(s, k, l).wait_recv()
            loads[k].start()
        for c in loads:
            c.wait()

        def col(i, _):
            cols = pl.ds(pl.multiple_of(i * NB, NB), NB)
            t = jnp.zeros((CG, NB), f32)
            for h in range(2):
                got = jnp.dot(putv[h], rb[:, cols], preferred_element_type=f32)
                t = t + got * jnp.concatenate([wqv[h]] * (NB // LANES), axis=1)
            pb[:, cols] = t.astype(bf)
            return 0

        lax.fori_loop(0, D // NB, col, 0, unroll=True)

        @pl.when(s == SELF)
        def _():
            pltpu.make_async_copy(pb, pr.at[b], lsem.at[0]).start()

        @pl.when(s < SELF)
        def _():
            pltpu.make_async_copy(pb, ps.at[s], lsem.at[0]).start()

    def send_back(s):
        pltpu.make_async_copy(pb, ps.at[s], lsem.at[0]).wait()

        @pl.when(s < SELF)
        def _():
            pcopy(s).start()

    def final_load(s):
        @pl.when(s < SELF)
        def _():
            precv(s).wait_recv()
        pltpu.make_async_copy(pr.at[grp_at(s)], fb, fsem.at[0]).start()

    def final(s):
        g = grp_at(s)
        pltpu.make_async_copy(pr.at[g], fb, fsem.at[0]).wait()
        code = jnp.sum(jnp.where(iota((T, LANES), 1) == g, cvec[...], 0.0), axis=1, keepdims=True)
        at = (iota((T, CG), 1) == code.astype(i32)).astype(f32).astype(bf)

        def col(i, _):
            cols = pl.ds(pl.multiple_of(i * NB, NB), NB)
            acc[:, cols] = acc[:, cols] + jnp.dot(at, fb[:, cols], preferred_element_type=f32)
            return 0

        lax.fori_loop(0, D // NB, col, 0, unroll=True)

    def step(s, _):
        @pl.when(s < G)
        def _():
            expert(s)

        @pl.when((s > 0) & (s <= G))
        def _():
            combine(s - 1)

        @pl.when(s >= LAG)
        def _():
            final_load(s - LAG)

        @pl.when((s > 0) & (s <= G))
        def _():
            send_back(s - 1)

        @pl.when(s >= LAG)
        def _():
            final(s - LAG)
        return 0

    lax.fori_loop(0, G + LAG, step, 0)

    def out(i, _):
        cols = pl.ds(pl.multiple_of(i * NB, NB), NB)
        xgv[:, cols] = acc[:, cols].astype(bf)
        return 0

    lax.fori_loop(0, D // NB, out, 0)
    run([pltpu.make_async_copy(xgv, y_ref, lsem.at[0])])

    for k in range(1, n):
        iy(k).wait_send()
    ag(1).wait_send()
    ag(n - 1).wait_send()
    fwd(0).wait_send()
    fwd(1).wait_send()
    for s in range(SELF):
        ix(s).wait_send()
        gxc(s).wait_send()
        for k in range(n):
            xcopy(s, k).wait_send()
        pcopy(s).wait_send()
    for s in range(G - 2, G):
        for l in range(EL):
            for k in range(1, n):
                ecopy(s, k, l).wait_send()


def solution(mesh):
    G = mesh.shape['grp']
    n = mesh.shape['ing']
    tok = P(('dp', 'grp', 'ing'), None)
    tok3 = P(('dp', 'grp', 'ing'), None, None)
    exp = P(('grp', 'ing'), None, None)

    def local(x, idx, g, w1, w3, w2, s1, s3, s2):
        T, D = x.shape
        _, M, KG = idx.shape
        K = M * KG
        EL, _, F = w1.shape
        E = EL * G * n
        C = (3 * T * K + 2 * E - 1) // (2 * E)
        CG = min(T, 3 * T * M // (2 * G))
        CB = EL * C
        R = n * CB
        flat = idx.reshape(T, K)
        it = flat.T
        gt = g.reshape(T, K).T
        anyspec = pl.BlockSpec(memory_space=pl.ANY)
        bf, f32, i32 = jnp.bfloat16, jnp.float32, jnp.int32
        sds = jax.ShapeDtypeStruct
        dma = lambda *s: pltpu.SemaphoreType.DMA(s)
        out = pl.pallas_call(
            functools.partial(_moe_kernel, G, n, EL, C, CG, T, D, F, K),
            out_shape=[sds((T, D), bf), sds((G, CG, D), bf), sds((n, T, D), bf), sds((n, G, CB, D), bf),
                       sds((G, n, CB, D), bf), sds((G, n, CB, D), bf),
                       sds((G, CG, D), bf)],
            in_specs=[anyspec] * 9,
            out_specs=[anyspec] * 7,
            scratch_shapes=[
                pltpu.VMEM((EL, D, F), bf), pltpu.VMEM((EL, D, F), bf), pltpu.VMEM((EL, F, D), bf),
                pltpu.VMEM((G * CB, D), bf), pltpu.VMEM((2, R, D), bf), pltpu.VMEM((R, D), bf),
                pltpu.VMEM((CG, D), bf), pltpu.VMEM((CG, D), bf), pltpu.VMEM((T, F), bf),
                pltpu.VMEM((T, D), bf), pltpu.VMEM((G * CB, T), bf),
                pltpu.VMEM((KG, CG, R), bf), pltpu.VMEM((KG, CG, LANES), f32),
                pltpu.VMEM((T, D), f32), pltpu.VMEM((T, T), bf), pltpu.VMEM((T, LANES), f32),
                pltpu.VMEM((n, K, T), i32), pltpu.VMEM((G, K, T), i32), pltpu.VMEM((G, K, T), f32),
                dma(n), dma(n), dma(n), dma(n), dma(G), dma(G), dma(G), dma(G),
                dma(G, n), dma(G, n), dma(G, EL * n), dma(G, EL * n), dma(G), dma(G), dma(G, EL),
                dma(G + n), dma(EL, 3), dma(1),
            ],
            compiler_params=pltpu.CompilerParams(
                collective_id=0, has_side_effects=True, vmem_limit_bytes=63 * 1024 * 1024),
            name="moe",
        )(x, it, gt, w1, w3, w2, s1, s3, s2)
        return out[0]

    return jax.shard_map(local, mesh=mesh, in_specs=(tok, tok3, tok3, exp, exp, exp, P(), P(), P()),
                         out_specs=tok, check_vma=False)
```

```python
import functools

import jax
import jax.numpy as jnp
from jax import lax
from jax.experimental import pallas as pl
from jax.experimental.pallas import tpu as pltpu
from jax.sharding import PartitionSpec as P

MESH = pl.DeviceIdType.MESH
LANES = 128


def _moe_kernel(G, n, EL, C, CG, T, D, F, K,
                x_ref, it_ref, gt_ref, w1_ref, w3_ref, w2_ref, s1_ref, s3_ref, s2_ref,
                y_ref, pr, xg, xs, xr, er, ps,
                W1, W3, W2, xb, eb, rb, pb, fb, hb, xgv, selv, putv, wqv, acc, tri, cvec,
                code, idxy, idxx, gx,
                agS, agR, iyS, iyR, ixS, ixR, gxS, gxR, xS, xR, eS, eR, pS, pR, oS, lsem, wsem, fsem):
    EG = EL * n
    CB = EL * C
    R = n * CB
    RE = n * C
    M = K // 2
    H = T // 2
    NB = min(512, D)
    LAG = 4
    SELF = G - 1
    bf = jnp.bfloat16
    f32 = jnp.float32
    i32 = jnp.int32
    d = lax.axis_index('dp')
    j = lax.axis_index('ing')
    b = lax.axis_index('grp')
    chips = G // 2
    chip, core = b // 2, b % 2

    def grp_at(s):
        t = s - (s // 4) * (2 * s - 7)
        dc = (t * (t + 1) // 2) % 4
        dcore = (s // 4 + 1 - (s % 7 + 6) // 7) % 2
        return 2 * ((chip + dc) % chips) + (core + dcore) % 2

    def inv(s):
        u = s % 4
        return s + (((u + 1) // 2) % 2) * (3 - 2 * u)

    def xdev(s):
        return (d, j, grp_at(s))

    def ydev(k):
        return (d, (j + k) % n, b)

    def iota(shape, dim):
        return lax.broadcasted_iota(i32, shape, dim)

    def remote(src, dst, ss, rs, dev):
        return pltpu.make_async_remote_copy(src_ref=src, dst_ref=dst, send_sem=ss, recv_sem=rs,
                                            device_id=dev, device_id_type=MESH)

    barrier = pltpu.get_barrier_semaphore()
    for k in range(1, n):
        pl.semaphore_signal(barrier, 1, device_id=ydev(k), device_id_type=MESH)
    for s in range(SELF):
        pl.semaphore_signal(barrier, 1, device_id=xdev(s), device_id_type=MESH)
    pl.semaphore_wait(barrier, n - 1 + G - 1)

    def ag(k):
        return remote(x_ref, xg.at[k], agS.at[k], agR.at[k], ydev(n - k))

    def fwd(h):
        k, dev = (1, n - 1) if h == 0 else (n - 1, 1)
        rows = pl.ds(h * H, H)
        return remote(xg.at[k, rows], xg.at[2, rows], agS.at[2 * h], agR.at[2 * h], ydev(dev))

    def iy(k):
        return remote(it_ref, idxy.at[k], iyS.at[k], iyR.at[k], ydev(n - k))

    def ix(s):
        return remote(it_ref, idxx.at[inv(s)], ixS.at[s], ixR.at[inv(s)], xdev(s))

    def ixrecv(s):
        return remote(it_ref, idxx.at[s], ixS.at[s], ixR.at[s], xdev(s))

    def gxc(s):
        return remote(gt_ref, gx.at[inv(s)], gxS.at[s], gxR.at[inv(s)], xdev(s))

    def gxrecv(s):
        return remote(gt_ref, gx.at[s], gxS.at[s], gxR.at[s], xdev(s))

    def xcopy(s, k):
        return remote(xs.at[k, s], xr.at[inv(s), k], xS.at[s, k], xR.at[inv(s), k], xdev(s))

    def xrecv(s, k):
        return remote(xs.at[k, s], xr.at[s, k], xS.at[s, k], xR.at[s, k], xdev(s))

    def erows(l, k):
        return pl.ds(pl.multiple_of(l * RE + k * C, 8), C)

    def lrows(l):
        return pl.ds(pl.multiple_of(l * C, 8), C)

    def ecopy(s, k, l):
        return remote(eb.at[s % 2, erows(l, k)], er.at[s, n - k, lrows(l)],
                      eS.at[s, l * n + k], eR.at[s, l * n + n - k], ydev(k))

    def erecv(s, k, l):
        return remote(eb.at[s % 2, erows(l, k)], er.at[s, k, lrows(l)],
                      eS.at[s, l * n + k], eR.at[s, l * n + k], ydev(k))

    def eown(s, l):
        return pltpu.make_async_copy(eb.at[s % 2, erows(l, 0)], er.at[s, 0, lrows(l)], oS.at[s, l])

    def pcopy(s):
        return remote(ps.at[s], pr.at[b], pS.at[s], pR.at[b], xdev(s))

    def precv(s):
        g = grp_at(s)
        return remote(ps.at[s], pr.at[g], pS.at[s], pR.at[g], xdev(s))

    def run(copies):
        for c in copies:
            c.start()
        for c in copies:
            c.wait()

    for k in range(1, n):
        iy(k).start()
    ag(1).start()
    ag(n - 1).start()

    def weights(l, shared):
        cols = pl.ds(l * F, F)
        srcs = ((s1_ref.at[:, cols], s3_ref.at[:, cols], s2_ref.at[cols]) if shared
                else (w1_ref.at[l], w3_ref.at[l], w2_ref.at[l]))
        return [pltpu.make_async_copy(s, w.at[l], wsem.at[l, i])
                for i, (s, w) in enumerate(zip(srcs, (W1, W3, W2)))]

    run([pltpu.make_async_copy(it_ref, idxy.at[0], lsem.at[0]),
         pltpu.make_async_copy(it_ref, idxx.at[SELF], lsem.at[1]),
         pltpu.make_async_copy(gt_ref, gx.at[SELF], lsem.at[2]),
         pltpu.make_async_copy(x_ref, xgv, lsem.at[4])])
    for s in range(SELF):
        ix(s).start()
        gxc(s).start()
    for l in range(EL):
        for c in weights(l, True):
            c.start()
    tri[...] = (iota((T, T), 0) < iota((T, T), 1)).astype(f32).astype(bf)

    def one_hot_rows(iv, eid):
        oh = iv[0:1, :] == eid
        for i in range(1, K):
            oh = oh | (iv[i:i + 1, :] == eid)
        return oh

    def gather(k, first, second):
        iv = idxy[k]
        r = iota((G * EL, T), 0)
        g_of = jnp.zeros((G * EL, T), i32)
        for q in range(1, G):
            g_of = g_of + (r >= q * EL).astype(i32)
        eid = g_of * (EG - EL) + r + j * EL
        oh = one_hot_rows(iv, eid)
        rank = jnp.dot(oh.astype(f32).astype(bf), tri[...], preferred_element_type=f32)
        code[...] = jnp.where(oh, rank.astype(i32), -(EL * C))
        row = iota((CB, T), 0)
        half = G // 2
        outs = [pltpu.make_async_copy(xb.at[pl.ds(s * CB, CB)], xr.at[SELF, k] if s == SELF else xs.at[k, s],
                                      lsem.at[s]) for s in range(G)]
        for h in range(2):
            for s in range(h * half, (h + 1) * half):
                base = grp_at(s) * EL
                want = code[pl.ds(base, 1), :]
                for l in range(1, EL):
                    want = jnp.where(row < l * C, want, code[pl.ds(base + l, 1), :] + l * C)
                selv[s * CB:(s + 1) * CB, :] = (row == want).astype(f32).astype(bf)
            if h == 1:
                for c in outs[:half]:
                    c.wait()
                for s in first:
                    xcopy(s, k).start()
            rows = pl.ds(h * half * CB, half * CB)

            def col(i, _):
                cols = pl.ds(pl.multiple_of(i * NB, NB), NB)
                xb[rows, cols] = jnp.dot(selv[rows, :], xgv[:, cols], preferred_element_type=f32).astype(bf)
                return 0

            lax.fori_loop(0, D // NB, col, 0, unroll=True)
            for c in outs[h * half:(h + 1) * half]:
                c.start()
        for c in outs[half:]:
            c.wait()
        for s in second:
            xcopy(s, k).start()

    def fetch(k):
        run([pltpu.make_async_copy(xg.at[k], xgv, lsem.at[0])])

    def up(l, src, rows, m):
        def body(i, _):
            cols = pl.ds(pl.multiple_of(i * LANES, LANES), LANES)
            w = jnp.concatenate([W1[l, :, cols], W3[l, :, cols]], axis=1)
            hh = jnp.dot(src[rows, :], w, preferred_element_type=f32)
            a, c = hh[:, :LANES], hh[:, LANES:]
            hb[0:m, cols] = (a * jax.nn.sigmoid(a) * c).astype(bf)
            return 0

        lax.fori_loop(0, F // LANES, body, 0, unroll=True)

    gather(0, (1, 2, 3, 0), (5, 6, 4))

    iv = idxy[0]
    gid = iota((2 * G, T), 0) * EG
    hit = jnp.zeros((2 * G, T), i32)
    for m in range(M):
        v = iv[2 * m:2 * m + 1, :]
        hit = hit + ((v >= gid) & (v < gid + EG)).astype(i32)
    below = jnp.dot(hit.astype(f32).astype(bf), tri[...], preferred_element_type=f32)
    place = jnp.where(hit > 0, below, -1.0)
    cvec[...] = jnp.concatenate([place, jnp.zeros((LANES - 2 * G, T), f32)], axis=0).T

    for l in range(EL):
        for c in weights(l, True):
            c.wait()
        up(l, xgv, pl.ds(0, T), T)

        def down(i, _):
            cols = pl.ds(pl.multiple_of(i * NB, NB), NB)
            t = jnp.dot(hb[...], W2[l, :, cols], preferred_element_type=f32)
            acc[:, cols] = t if l == 0 else acc[:, cols] + t
            return 0

        lax.fori_loop(0, D // NB, down, 0, unroll=True)
        for c in weights(l, False):
            c.start()

    for k in (1, n - 1):
        iy(k).wait_recv()
        ag(k).wait_recv()
        fwd(0 if k == 1 else 1).start()
        fetch(k)
        gather(k, (0, 1, 2, 3), ())
    iy(2).wait_recv()
    fwd(0).wait_recv()
    fwd(1).wait_recv()
    fetch(2)
    gather(2, (0, 1, 2, 3), ())
    for s in range(4, SELF):
        for k in range(1, n):
            xcopy(s, k).start()
    for l in range(EL):
        for c in weights(l, False):
            c.wait()
    for s in range(SELF):
        ixrecv(s).wait_recv()
        gxrecv(s).wait_recv()

    def expert(s):
        @pl.when(s < SELF)
        def _():
            for k in range(n):
                xrecv(s, k).wait_recv()

        def load(l, k):
            return pltpu.make_async_copy(xr.at[s, k, lrows(l)], xb.at[erows(l, k)], lsem.at[l * n + k])

        for l in range(EL):
            for k in range(n):
                load(l, k).start()

        @pl.when(s >= 2)
        def _():
            for l in range(EL):
                for k in range(1, n):
                    ecopy(s - 2, k, l).wait_send()

        def one(l, _):
            for k in range(n):
                load(l, k).wait()
            rows = pl.ds(pl.multiple_of(l * RE, 8), RE)
            up(l, xb, rows, RE)

            def down(i, _):
                cols = pl.ds(pl.multiple_of(i * NB, NB), NB)
                eb[s % 2, rows, cols] = jnp.dot(hb[0:RE, :], W2[l, :, cols], preferred_element_type=f32).astype(bf)
                return 0

            lax.fori_loop(0, D // NB, down, 0, unroll=True)
            for k in (1, n - 1, 2):
                ecopy(s, k, l).start()
            eown(s, l).start()
            return 0

        lax.fori_loop(0, EL, one, 0)

    def combine(s):
        iv, gv = idxx[s], gx[s]
        r = iota((2 * EG, T), 0)
        oh = one_hot_rows(iv, r + b * EG) & (r < EG)
        mine = [(iv[2 * m:2 * m + 1, :] >= b * EG) & (iv[2 * m:2 * m + 1, :] < b * EG + EG) for m in range(M)]
        hit = mine[0]
        for m in range(1, M):
            hit = hit | mine[m]
        ohf = jnp.where(r == EG, hit.astype(f32), oh.astype(f32))
        cnt = jnp.dot(ohf.astype(bf), tri[...], preferred_element_type=f32).astype(i32)
        slot = jnp.where(hit, cnt[EG:EG + 1, :], -1)
        jd = jnp.zeros((2 * EG, T), i32)
        for q in range(1, n):
            jd = jd + (r >= q * EL).astype(i32)
        kk = jd - j
        kk = jnp.where(kk < 0, kk + n, kk)
        place = kk * CB + (r - jd * EL) * C + cnt
        at = iota((CG, T), 0) == slot
        atb = at.astype(f32).astype(bf)
        for i in range(2):
            ei = jnp.zeros((1, T), i32)
            gi = jnp.zeros((1, T), f32)
            for m in range(M):
                ei = ei + jnp.where(mine[m], iv[2 * m + i:2 * m + i + 1, :], 0)
                gi = gi + jnp.where(mine[m], gv[2 * m + i:2 * m + i + 1, :], 0.0)
            row = jnp.sum(jnp.where((r + b * EG == ei) & (r < EG), place, 0), axis=0, keepdims=True)
            row = jnp.where(hit, row, -1)
            inrow = (iota((R, T), 0) == row).astype(f32).astype(bf)
            putv[i] = lax.dot_general(atb, inrow, (((1,), (1,)), ((), ())), preferred_element_type=f32).astype(bf)
            w = jnp.sum(jnp.where(at, gi, 0.0), axis=1, keepdims=True)
            wqv[i] = jnp.broadcast_to(w, (CG, LANES))
        loads = [pltpu.make_async_copy(er.at[s, k], rb.at[pl.ds(k * CB, CB)], lsem.at[k]) for k in range(n)]
        for l in range(EL):
            eown(s, l).wait()
        loads[0].start()
        for k in (1, n - 1, 2):
            for l in range(EL):
                erecv(s, k, l).wait_recv()
            loads[k].start()
        for c in loads:
            c.wait()

        def col(i, _):
            cols = pl.ds(pl.multiple_of(i * NB, NB), NB)
            t = jnp.zeros((CG, NB), f32)
            for h in range(2):
                got = jnp.dot(putv[h], rb[:, cols], preferred_element_type=f32)
                t = t + got * jnp.concatenate([wqv[h]] * (NB // LANES), axis=1)
            pb[:, cols] = t.astype(bf)
            return 0

        lax.fori_loop(0, D // NB, col, 0, unroll=True)

        @pl.when(s == SELF)
        def _():
            pltpu.make_async_copy(pb, pr.at[b], lsem.at[0]).start()

        @pl.when(s < SELF)
        def _():
            pltpu.make_async_copy(pb, ps.at[s], lsem.at[0]).start()

    def send_back(s):
        pltpu.make_async_copy(pb, ps.at[s], lsem.at[0]).wait()

        @pl.when(s < SELF)
        def _():
            pcopy(s).start()

    def final_load(s):
        @pl.when(s < SELF)
        def _():
            precv(s).wait_recv()
        pltpu.make_async_copy(pr.at[grp_at(s)], fb, fsem.at[0]).start()

    def final(s):
        g = grp_at(s)
        pltpu.make_async_copy(pr.at[g], fb, fsem.at[0]).wait()
        own = jnp.sum(jnp.where(iota((T, LANES), 1) == g, cvec[...], 0.0), axis=1, keepdims=True)
        at = (iota((T, CG), 1) == own.astype(i32)).astype(f32).astype(bf)

        def col(i, _):
            cols = pl.ds(pl.multiple_of(i * NB, NB), NB)
            acc[:, cols] = acc[:, cols] + jnp.dot(at, fb[:, cols], preferred_element_type=f32)
            return 0

        lax.fori_loop(0, D // NB, col, 0, unroll=True)

    def turn(f):
        return f + (f // 5) * (2 - 3 * ((f - 4) // 2))

    def step(s, _):
        @pl.when(s < G)
        def _():
            expert(s)

        @pl.when((s > 0) & (s <= G))
        def _():
            combine(s - 1)

        @pl.when(s >= LAG)
        def _():
            final_load(turn(s - LAG))

        @pl.when((s > 0) & (s <= G))
        def _():
            send_back(s - 1)

        @pl.when(s >= LAG)
        def _():
            final(turn(s - LAG))
        return 0

    lax.fori_loop(0, G + LAG, step, 0)

    def out(i, _):
        cols = pl.ds(pl.multiple_of(i * NB, NB), NB)
        xgv[:, cols] = acc[:, cols].astype(bf)
        return 0

    lax.fori_loop(0, D // NB, out, 0)
    run([pltpu.make_async_copy(xgv, y_ref, lsem.at[0])])

    for k in range(1, n):
        iy(k).wait_send()
    ag(1).wait_send()
    ag(n - 1).wait_send()
    fwd(0).wait_send()
    fwd(1).wait_send()
    for s in range(SELF):
        ix(s).wait_send()
        gxc(s).wait_send()
        for k in range(n):
            xcopy(s, k).wait_send()
        pcopy(s).wait_send()
    for s in range(G - 2, G):
        for l in range(EL):
            for k in range(1, n):
                ecopy(s, k, l).wait_send()


def solution(mesh):
    G = mesh.shape['grp']
    n = mesh.shape['ing']
    tok = P(('dp', 'grp', 'ing'), None)
    tok3 = P(('dp', 'grp', 'ing'), None, None)
    exp = P(('grp', 'ing'), None, None)

    def local(x, idx, g, w1, w3, w2, s1, s3, s2):
        T, D = x.shape
        _, M, KG = idx.shape
        K = M * KG
        EL, _, F = w1.shape
        E = EL * G * n
        C = (3 * T * K + 2 * E - 1) // (2 * E)
        CG = min(T, 3 * T * M // (2 * G))
        CB = EL * C
        R = n * CB
        flat = idx.reshape(T, K)
        it = flat.T
        gt = g.reshape(T, K).T
        anyspec = pl.BlockSpec(memory_space=pl.ANY)
        bf, f32, i32 = jnp.bfloat16, jnp.float32, jnp.int32
        sds = jax.ShapeDtypeStruct
        dma = lambda *s: pltpu.SemaphoreType.DMA(s)
        out = pl.pallas_call(
            functools.partial(_moe_kernel, G, n, EL, C, CG, T, D, F, K),
            out_shape=[sds((T, D), bf), sds((G, CG, D), bf), sds((n, T, D), bf), sds((n, G, CB, D), bf),
                       sds((G, n, CB, D), bf), sds((G, n, CB, D), bf),
                       sds((G, CG, D), bf)],
            in_specs=[anyspec] * 9,
            out_specs=[anyspec] * 7,
            scratch_shapes=[
                pltpu.VMEM((EL, D, F), bf), pltpu.VMEM((EL, D, F), bf), pltpu.VMEM((EL, F, D), bf),
                pltpu.VMEM((G * CB, D), bf), pltpu.VMEM((2, R, D), bf), pltpu.VMEM((R, D), bf),
                pltpu.VMEM((CG, D), bf), pltpu.VMEM((CG, D), bf), pltpu.VMEM((T, F), bf),
                pltpu.VMEM((T, D), bf), pltpu.VMEM((G * CB, T), bf),
                pltpu.VMEM((KG, CG, R), bf), pltpu.VMEM((KG, CG, LANES), f32),
                pltpu.VMEM((T, D), f32), pltpu.VMEM((T, T), bf), pltpu.VMEM((T, LANES), f32),
                pltpu.VMEM((G * EL, T), i32), pltpu.VMEM((n, K, T), i32), pltpu.VMEM((G, K, T), i32), pltpu.VMEM((G, K, T), f32),
                dma(n), dma(n), dma(n), dma(n), dma(G), dma(G), dma(G), dma(G),
                dma(G, n), dma(G, n), dma(G, EL * n), dma(G, EL * n), dma(G), dma(G), dma(G, EL),
                dma(G + n), dma(EL, 3), dma(1),
            ],
            compiler_params=pltpu.CompilerParams(
                collective_id=0, has_side_effects=True, vmem_limit_bytes=63 * 1024 * 1024),
            name="moe",
        )(x, it, gt, w1, w3, w2, s1, s3, s2)
        return out[0]

    return jax.shard_map(local, mesh=mesh, in_specs=(tok, tok3, tok3, exp, exp, exp, P(), P(), P()),
                         out_specs=tok, check_vma=False)
```
